16 devices in a mesh: data: 4 (over z, y), tp: 4 (over x, core).
Axes of the slice: x: 2, y: 2, z: 2, core: 2. Of those that a mesh axis runs over, the one named last changes fastest.
Arguments:
- x_in: bfloat16 [16384, 4096], P('data'), parts along dimension 0
- w_gate: bfloat16 [4096, 14336], P(None, 'tp')
- w_up: bfloat16 [4096, 14336], P(None, 'tp')
- w_down: bfloat16 [14336, 4096], P('tp')
- residual: bfloat16 [16384, 4096], P(('data', 'tp')), parts along dimension 0
- norm_gain: float32 [4096], replicated
Outputs:
- output 1: bfloat16 [16384, 4096], P(('data', 'tp')), parts along dimension 0
- output 2: bfloat16 [16384, 4096], P(('data', 'tp')), parts along dimension 0
There are 4 independent parts. The reference program is written for one: setup_inputs(seed, part) draws one part's arguments, and reference() takes and returns one part's arrays. A program takes and returns all parts, laid end to end along the dimension named above; an argument that names none is the same for every part.
All inputs are finite; a program needn't handle non-finite values.
Results may differ from the reference program's by a relative error of at most 0.00659775.
Values are sent between devices in bfloat16 or wider.
A program may use at most 1 GiB of HBM per device.

```python
import jax
import jax.numpy as jnp
from jax import lax

T = 4096
D = 4096
F = 14336
TP = 4
F_SHARD = F // TP
EPS = 1e-5


def setup_inputs(seed: int = 0, part: int = 0) -> dict:
    key = jax.random.key(seed)
    shared = jax.random.split(key, 4)
    local = jax.random.split(jax.random.fold_in(key, part), 2)
    x_in = jax.random.normal(local[0], (T, D), jnp.float32).astype(jnp.bfloat16)
    residual = jax.random.normal(local[1], (T, D), jnp.float32).astype(jnp.bfloat16)
    w_gate = (jax.random.normal(shared[0], (D, F), jnp.float32) * D ** -0.5).astype(jnp.bfloat16)
    w_up = (jax.random.normal(shared[1], (D, F), jnp.float32) * D ** -0.5).astype(jnp.bfloat16)
    w_down = (jax.random.normal(shared[2], (F, D), jnp.float32) * (2.0 / F) ** 0.5).astype(jnp.bfloat16)
    norm_gain = 1.0 + 0.3 * jax.random.normal(shared[3], (D,), jnp.float32)
    return {"x_in": x_in, "w_gate": w_gate, "w_up": w_up, "w_down": w_down, "residual": residual, "norm_gain": norm_gain}


def reference(x_in, w_gate, w_up, w_down, residual, norm_gain):
    gate_shards = w_gate.reshape(D, TP, F_SHARD).transpose(1, 0, 2)
    up_shards = w_up.reshape(D, TP, F_SHARD).transpose(1, 0, 2)
    down_shards = w_down.reshape(TP, F_SHARD, D)

    def add_shard(running, shard_w):
        gate_cols, up_cols, down_rows = shard_w
        gate_val = jnp.dot(x_in, gate_cols, preferred_element_type=jnp.float32)
        up_val = jnp.dot(x_in, up_cols, preferred_element_type=jnp.float32)
        hidden = (jax.nn.silu(gate_val) * up_val).astype(jnp.bfloat16)
        part_prod = jnp.dot(hidden, down_rows, preferred_element_type=jnp.float32).astype(jnp.bfloat16)
        return running + part_prod.astype(jnp.float32), None

    y_sum = lax.scan(add_shard, jnp.zeros((T, D), jnp.float32), (gate_shards, up_shards, down_shards))[0]
    hidden_sum = residual.astype(jnp.float32) + y_sum
    mean_sq = jnp.mean(hidden_sum * hidden_sum, axis=-1, keepdims=True)
    normed = hidden_sum * lax.rsqrt(mean_sq + EPS) * norm_gain
    return hidden_sum.astype(jnp.bfloat16), normed.astype(jnp.bfloat16)
```

```python
import functools

import jax
import jax.numpy as jnp
from jax import lax
from jax.experimental import pallas as pl
from jax.experimental.pallas import tpu as pltpu
from jax.sharding import PartitionSpec as P

EPS = 1e-5
TP = 4
M = 512
NG = 512
ND = 512
SUB = 256
FB = 64
ROWS = 16
TAIL = 4

bf16 = jnp.bfloat16
f32 = jnp.float32


def kernel(x_hbm, wg_hbm, wu_hbm, wd_hbm, res_hbm, gain_ref,
           h_hbm, n_hbm, y_hbm, r_hbm,
           x_v, wg_v, wu_v, wd_v, g_v, y_v, in_v, out_v,
           x_sem, wg_sem, wu_sem, wd_sem, y_sem, in_sem, out_sem,
           send_sem, recv_sem, tsend_sem, trecv_sem):
    D, FS = wg_hbm.shape
    R = res_hbm.shape[0]
    HALVES = R // M
    assert HALVES == 2
    n_gu, n_dn = FS // NG, D // ND
    n_chunk = TP * HALVES
    me = lax.axis_index("tp")
    far_same = lax.rem(me + 2, TP)
    far_other = TP - 1 - me
    near = me + 1 - 2 * lax.rem(me, 2)
    peers = (far_same, far_other, near)

    barrier = pltpu.get_barrier_semaphore()
    for peer in peers:
        pl.semaphore_signal(barrier, inc=1, device_id={"tp": peer}, device_id_type=pl.DeviceIdType.MESH)
    pl.semaphore_wait(barrier, TP - 1)

    def slot_of(c):
        late = c // 4
        return (1 - late) * lax.rem(c, 2) + late * (2 + (c - 4) // 2)

    def half_of(c):
        late = c // 4
        return (1 - late) * (c // 2) + late * lax.rem(c, 2)

    def owner_of(c):
        late = c // 4
        odd = lax.rem(c, 2)
        far = (1 - odd) * far_same + odd * far_other
        own = (c - 4) // 2
        close = (1 - own) * near + own * me
        return (1 - late) * far + late * close

    def x_copy(c):
        row = pl.multiple_of(owner_of(c) * R + half_of(c) * M, M)
        return pltpu.make_async_copy(x_hbm.at[pl.ds(row, M), :], x_v, x_sem)

    def gu_copies(j, s):
        col = pl.multiple_of(j * NG, NG)
        return (pltpu.make_async_copy(wg_hbm.at[:, pl.ds(col, NG)], wg_v.at[s], wg_sem.at[s]),
                pltpu.make_async_copy(wu_hbm.at[:, pl.ds(col, NG)], wu_v.at[s], wu_sem.at[s]))

    def wd_copy(d, s):
        col = pl.multiple_of(d * ND, ND)
        return pltpu.make_async_copy(wd_hbm.at[:, pl.ds(col, ND)], wd_v.at[s], wd_sem.at[s])

    def y_copy(c, d):
        row = pl.multiple_of(half_of(c) * M, M)
        col = pl.multiple_of(d * ND, ND)
        s = lax.rem(d, 2)
        return pltpu.make_async_copy(y_v.at[s], y_hbm.at[slot_of(c), pl.ds(row, M), pl.ds(col, ND)], y_sem.at[s])

    def remote(slot, row, rows, cols, ssem, rsem):
        ref = (slot, pl.ds(row, rows)) + ((cols,) if cols is not None else (slice(None),))
        return pltpu.make_async_remote_copy(
            src_ref=y_hbm.at[ref], dst_ref=r_hbm.at[ref], send_sem=ssem, recv_sem=rsem,
            device_id={"tp": peers[slot]}, device_id_type=pl.DeviceIdType.MESH)

    def chunk_copy(c):
        slot = (0, 1, 0, 1, 2, 2)[c]
        half = (0, 0, 1, 1, 0, 1)[c]
        return remote(slot, half * M, M, None, send_sem.at[c], recv_sem.at[c])

    def first_piece(d):
        col = pl.multiple_of(d * ND, ND)
        return remote(0, 0, M, pl.ds(col, ND), send_sem.at[0], recv_sem.at[0])

    def tail_piece(t):
        rows = M // TAIL
        return remote(1, M + t * rows, rows, None, tsend_sem.at[t], trecv_sem.at[t])

    def send_chunk(c):
        if c == 3:
            for t in range(TAIL):
                tail_piece(t).start()
        else:
            chunk_copy(c).start()

    x_copy(0).start()
    for cp in gu_copies(0, 0):
        cp.start()

    def chunk(c, _):
        x_copy(c).wait()

        def gu_step(j, _):
            g = c * n_gu + j
            s = lax.rem(g, 2)

            @pl.when(j + 1 < n_gu)
            def _():
                for cp in gu_copies(j + 1, 1 - s):
                    cp.start()

            @pl.when(j == n_gu - 3)
            def _():
                wd_copy(0, 0).start()

            @pl.when(j == n_gu - 2)
            def _():
                wd_copy(1, 1).start()

            for cp in gu_copies(j, s):
                cp.wait()
            for q in range(NG // SUB):
                cols = slice(q * SUB, (q + 1) * SUB)
                gate = jnp.dot(x_v[...], wg_v[s, :, cols], preferred_element_type=f32)
                up = jnp.dot(x_v[...], wu_v[s, :, cols], preferred_element_type=f32)
                hid = (gate * jax.nn.sigmoid(gate) * up).astype(bf16)
                g_v[:, pl.ds(pl.multiple_of(j * NG + q * SUB, SUB), SUB)] = hid
            return 0

        lax.fori_loop(0, n_gu, gu_step, 0)

        def dn_step(d, _):
            @pl.when(d + 2 < n_dn)
            def _():
                wd_copy(d + 2, lax.rem(d + 2, 3)).start()

            @pl.when((d == 2) & (c + 1 < n_chunk))
            def _():
                x_copy(c + 1).start()

            @pl.when((d == 4) & (c + 1 < n_chunk))
            def _():
                for cp in gu_copies(0, lax.rem((c + 1) * n_gu, 2)):
                    cp.start()

            wd_copy(d, lax.rem(d, 3)).wait()

            @pl.when(d >= 1)
            def _():
                y_copy(c, d - 1).wait()

            @pl.when((d >= 1) & (c == 0))
            def _():
                first_piece(d - 1).start()

            y = jnp.dot(g_v[...], wd_v[lax.rem(d, 3)], preferred_element_type=f32)
            y_v[lax.rem(d, 2)] = y.astype(bf16)
            y_copy(c, d).start()
            return 0

        lax.fori_loop(0, n_dn, dn_step, 0)
        y_copy(c, n_dn - 1).wait()

        @pl.when(c == 0)
        def _():
            first_piece(n_dn - 1).start()

        for k in range(1, 6):
            @pl.when(c == k)
            def _(k=k):
                send_chunk(k)
        return 0

    lax.fori_loop(0, n_chunk, chunk, 0)

    def in_copies(b, s):
        row = pl.multiple_of(b * FB, FB)
        out = [pltpu.make_async_copy(res_hbm.at[pl.ds(row, FB), :], in_v.at[s, 0], in_sem.at[s, 0]),
               pltpu.make_async_copy(y_hbm.at[3, pl.ds(row, FB), :], in_v.at[s, 1], in_sem.at[s, 1])]
        for k in range(3):
            out.append(pltpu.make_async_copy(r_hbm.at[k, pl.ds(row, FB), :], in_v.at[s, 2 + k], in_sem.at[s, 2 + k]))
        return out

    def out_copies(b, s):
        row = pl.multiple_of(b * FB, FB)
        return (pltpu.make_async_copy(out_v.at[s, 0], h_hbm.at[pl.ds(row, FB), :], out_sem.at[s, 0]),
                pltpu.make_async_copy(out_v.at[s, 1], n_hbm.at[pl.ds(row, FB), :], out_sem.at[s, 1]))

    n_fb = R // FB
    per_tail = M // TAIL // FB

    def need(b):
        @pl.when(b == n_fb // 2)
        def _():
            for c in (2, 5):
                chunk_copy(c).wait_recv()
        for t in range(TAIL):
            @pl.when(b == n_fb // 2 + t * per_tail)
            def _(t=t):
                tail_piece(t).wait_recv()

    for c in (0, 1, 4):
        chunk_copy(c).wait_recv()
    for cp in in_copies(0, 0):
        cp.start()

    def final(b, _):
        s = lax.rem(b, 2)
        need(b + 1)

        @pl.when(b + 1 < n_fb)
        def _():
            for cp in in_copies(b + 1, 1 - s):
                cp.start()

        for cp in in_copies(b, s):
            cp.wait()

        @pl.when(b >= 2)
        def _():
            for cp in out_copies(b - 2, s):
                cp.wait()

        def rows_step(i, _):
            rows = pl.ds(pl.multiple_of(i * ROWS, ROWS), ROWS)
            h = in_v[s, 0, rows, :].astype(f32)
            y = in_v[s, 1, rows, :].astype(f32)
            for k in range(3):
                y = y + in_v[s, 2 + k, rows, :].astype(f32)
            h = h + y
            mean_sq = jnp.mean(h * h, axis=-1, keepdims=True)
            out_v[s, 0, rows, :] = h.astype(bf16)
            out_v[s, 1, rows, :] = (h * lax.rsqrt(mean_sq + EPS) * gain_ref[...]).astype(bf16)
            return 0

        lax.fori_loop(0, FB // ROWS, rows_step, 0)
        for cp in out_copies(b, s):
            cp.start()
        return 0

    lax.fori_loop(0, n_fb, final, 0)
    for b in (n_fb - 2, n_fb - 1):
        for cp in out_copies(b, b % 2):
            cp.wait()
    for c in (0, 1, 2, 4, 5):
        chunk_copy(c).wait_send()
    for t in range(TAIL):
        tail_piece(t).wait_send()


def solution(mesh):
    def local_block(x_in, w_gate, w_up, w_down, residual, norm_gain):
        T, D = x_in.shape
        FS = w_gate.shape[1]
        R = residual.shape[0]
        any_ = pl.BlockSpec(memory_space=pl.ANY)
        h_out, n, _, _ = pl.pallas_call(
            kernel,
            out_shape=(jax.ShapeDtypeStruct((R, D), bf16), jax.ShapeDtypeStruct((R, D), bf16),
                       jax.ShapeDtypeStruct((TP, R, D), bf16), jax.ShapeDtypeStruct((TP - 1, R, D), bf16)),
            in_specs=[any_] * 5 + [pl.BlockSpec(memory_space=pltpu.VMEM)],
            out_specs=(any_,) * 4,
            scratch_shapes=[
                pltpu.VMEM((M, D), bf16),
                pltpu.VMEM((2, D, NG), bf16),
                pltpu.VMEM((2, D, NG), bf16),
                pltpu.VMEM((3, FS, ND), bf16),
                pltpu.VMEM((M, FS), bf16),
                pltpu.VMEM((2, M, ND), bf16),
                pltpu.VMEM((2, 5, FB, D), bf16),
                pltpu.VMEM((2, 2, FB, D), bf16),
                pltpu.SemaphoreType.DMA,
                pltpu.SemaphoreType.DMA((2,)),
                pltpu.SemaphoreType.DMA((2,)),
                pltpu.SemaphoreType.DMA((3,)),
                pltpu.SemaphoreType.DMA((2,)),
                pltpu.SemaphoreType.DMA((2, 5)),
                pltpu.SemaphoreType.DMA((2, 2)),
                pltpu.SemaphoreType.DMA((6,)),
                pltpu.SemaphoreType.DMA((6,)),
                pltpu.SemaphoreType.DMA((TAIL,)),
                pltpu.SemaphoreType.DMA((TAIL,)),
            ],
            compiler_params=pltpu.CompilerParams(collective_id=0, has_side_effects=True, vmem_limit_bytes=60 * 1024 * 1024),
            name="mlp_block",
        )(x_in, w_gate, w_up, w_down, residual, norm_gain.reshape(1, D))
        return h_out, n

    row_spec = P(("data", "tp"), None)
    return jax.shard_map(local_block, mesh=mesh, in_specs=(P("data", None), P(None, "tp"), P(None, "tp"), P("tp", None), row_spec, P(None)), out_specs=(row_spec, row_spec), check_vma=False)
```

```python
import jax
import jax.numpy as jnp
from jax import lax
from jax.experimental import pallas as pl
from jax.experimental.pallas import tpu as pltpu
from jax.sharding import PartitionSpec as P

EPS = 1e-5
TP = 4
M = 512
SUB = 256
ND = 512
BIG = 1024
TAIL = 4
FB = 256
ROWS = 8

bf16 = jnp.bfloat16
f32 = jnp.float32


def matmul_kernel(x_hbm, wg_hbm, wu_hbm, wd_hbm, y_hbm, r_hbm,
                  x_v, wg_v, wu_v, wd_v, g_v, y_v,
                  x_sem, wg_sem, wu_sem, wd_sem, y_sem, send_sem, recv_sem):
    D, FS = wg_hbm.shape
    R = y_hbm.shape[1]
    assert R == 2 * M and R == BIG
    n_gu, n_dn = FS // (2 * SUB), D // ND
    me = lax.axis_index("tp")
    far_same = lax.rem(me + 2, TP)
    far_other = TP - 1 - me
    near = me + 1 - 2 * lax.rem(me, 2)
    peers = (far_same, far_other, near)

    barrier = pltpu.get_barrier_semaphore()
    for peer in peers:
        pl.semaphore_signal(barrier, inc=1, device_id={"tp": peer}, device_id_type=pl.DeviceIdType.MESH)
    pl.semaphore_wait(barrier, TP - 1)

    def owner_of(c):
        own = c // 2
        mid = (1 - own) * ((1 - c) * far_other + c * near)
        return mid + own * me

    def x_small(c):
        row = pl.multiple_of(far_same * R + c * M, M)
        return pltpu.make_async_copy(x_hbm.at[pl.ds(row, M), :], x_v.at[pl.ds(0, M), :], x_sem)

    def x_big(c):
        row = pl.multiple_of(owner_of(c) * R, BIG)
        return pltpu.make_async_copy(x_hbm.at[pl.ds(row, BIG), :], x_v, x_sem)

    def gu_copies(j, slot):
        col = pl.ds(pl.multiple_of(j * 2 * SUB, 2 * SUB), 2 * SUB)
        return (pltpu.make_async_copy(wg_hbm.at[:, col], wg_v.at[slot], wg_sem.at[slot]),
                pltpu.make_async_copy(wu_hbm.at[:, col], wu_v.at[slot], wu_sem.at[slot]))

    def dn_copy(d):
        k = lax.rem(d, 4)
        at = pl.ds(pl.multiple_of(lax.rem(k, 2) * ND, ND), ND)
        return pltpu.make_async_copy(wd_hbm.at[:, pl.ds(pl.multiple_of(d * ND, ND), ND)], wd_v.at[k // 2, :, at], wd_sem.at[k])

    def dn_big(d):
        k = lax.rem(d, 2)
        return pltpu.make_async_copy(wd_hbm.at[:, pl.ds(pl.multiple_of(d * BIG, BIG), BIG)], wd_v.at[k], wd_sem.at[k])

    def y_small(c, d):
        k = lax.rem(d, 2)
        return pltpu.make_async_copy(
            y_v.at[k, pl.ds(0, M), pl.ds(0, ND)],
            y_hbm.at[0, pl.ds(pl.multiple_of(c * M, M), M), pl.ds(pl.multiple_of(d * ND, ND), ND)], y_sem.at[k])

    def y_big(c, d):
        k = lax.rem(d, 2)
        return pltpu.make_async_copy(y_v.at[k], y_hbm.at[c + 1, :, pl.ds(pl.multiple_of(d * BIG, BIG), BIG)], y_sem.at[k])

    def remote(slot, row, rows, cols, ssem, rsem):
        ref = (slot, pl.ds(row, rows), slice(None) if cols is None else cols)
        return pltpu.make_async_remote_copy(
            src_ref=y_hbm.at[ref], dst_ref=r_hbm.at[ref], send_sem=ssem, recv_sem=rsem,
            device_id={"tp": peers[slot]}, device_id_type=pl.DeviceIdType.MESH)

    def first_piece(d):
        return remote(0, 0, M, pl.ds(pl.multiple_of(d * ND, ND), ND), send_sem.at[0], recv_sem.at[0])

    rows = R // TAIL
    copies = [remote(0, M, M, None, send_sem.at[1], recv_sem.at[1])]
    copies += [remote(1, t * rows, rows, None, send_sem.at[2 + t], recv_sem.at[2 + t]) for t in range(TAIL)]
    copies += [remote(2, 0, R, None, send_sem.at[2 + TAIL], recv_sem.at[2 + TAIL])]
    first_whole = remote(0, 0, M, None, send_sem.at[0], recv_sem.at[0])

    def hidden(m, slot, j):
        for q in range(2):
            cols = slice(q * SUB, (q + 1) * SUB)
            for r in range(m // M):
                part = slice(r * M, (r + 1) * M)
                gate = jnp.dot(x_v[part, :], wg_v[slot, :, cols], preferred_element_type=f32)
                up = jnp.dot(x_v[part, :], wu_v[slot, :, cols], preferred_element_type=f32)
                g_v[part, pl.ds(pl.multiple_of(j * 2 * SUB + q * SUB, SUB), SUB)] = (gate * jax.nn.sigmoid(gate) * up).astype(bf16)

    def gate_up(m, base, before):
        def gu_step(j, _):
            slot = lax.rem(base + j, 2)

            @pl.when(j + 1 < n_gu)
            def _():
                for cp in gu_copies(j + 1, 1 - slot):
                    cp.start()

            before(j)
            for cp in gu_copies(j, slot):
                cp.wait()
            hidden(m, slot, j)
            return 0

        lax.fori_loop(0, n_gu, gu_step, 0)

    def small_chunk(c, _):
        x_small(c).wait()

        def before(j):
            @pl.when(j >= n_gu - 3)
            def _():
                dn_copy(j - (n_gu - 3)).start()

        gate_up(M, c * n_gu, before)

        def dn_step(d, _):
            @pl.when(d + 3 < n_dn)
            def _():
                dn_copy(d + 3).start()

            @pl.when((d == 1) & (c == 0))
            def _():
                x_small(1).start()

            @pl.when((d == 1) & (c == 1))
            def _():
                x_big(0).start()

            @pl.when(d == 3)
            def _():
                for cp in gu_copies(0, lax.rem((c + 1) * n_gu, 2)):
                    cp.start()

            dn_copy(d).wait()

            @pl.when(d >= 1)
            def _():
                y_small(c, d - 1).wait()

            @pl.when((d >= 1) & (c == 0))
            def _():
                first_piece(d - 1).start()

            k = lax.rem(d, 4)
            at = pl.multiple_of(lax.rem(k, 2) * ND, ND)
            y = jnp.dot(g_v[0:M, :], wd_v[k // 2, :, pl.ds(at, ND)], preferred_element_type=f32)
            y_v[lax.rem(d, 2), 0:M, 0:ND] = y.astype(bf16)
            y_small(c, d).start()
            return 0

        lax.fori_loop(0, n_dn, dn_step, 0)
        y_small(c, n_dn - 1).wait()

        @pl.when(c == 0)
        def _():
            first_piece(n_dn - 1).start()

        @pl.when(c == 1)
        def _():
            copies[0].start()
        return 0

    n_big = TP - 1
    n_wide = D // BIG

    def big_chunk(c, _):
        x_big(c).wait()

        def before(j):
            @pl.when(j == n_gu - 2)
            def _():
                dn_big(0).start()

        gate_up(BIG, c * n_gu, before)

        def dn_step(d, _):
            @pl.when(d + 1 < n_wide)
            def _():
                dn_big(d + 1).start()

            @pl.when((d == 1) & (c + 1 < n_big))
            def _():
                x_big(c + 1).start()

            @pl.when((d == 2) & (c + 1 < n_big))
            def _():
                for cp in gu_copies(0, lax.rem((c + 1) * n_gu, 2)):
                    cp.start()

            dn_big(d).wait()

            @pl.when(d >= 1)
            def _():
                y_big(c, d - 1).wait()

            k = lax.rem(d, 2)
            for r in range(BIG // M):
                part = slice(r * M, (r + 1) * M)
                for q in range(BIG // ND):
                    cols = slice(q * ND, (q + 1) * ND)
                    y = jnp.dot(g_v[part, :], wd_v[k, :, cols], preferred_element_type=f32)
                    y_v[k, part, cols] = y.astype(bf16)
            y_big(c, d).start()
            return 0

        lax.fori_loop(0, n_wide, dn_step, 0)
        y_big(c, n_wide - 1).wait()

        @pl.when(c == 0)
        def _():
            for cp in copies[1:1 + TAIL]:
                cp.start()

        @pl.when(c == 1)
        def _():
            copies[1 + TAIL].start()
        return 0

    for cp in gu_copies(0, 0):
        cp.start()
    x_small(0).start()
    lax.fori_loop(0, 2, small_chunk, 0)
    lax.fori_loop(0, n_big, big_chunk, 0)
    for cp in [first_whole] + copies:
        cp.wait_recv()
    for cp in [first_whole] + copies:
        cp.wait_send()


def norm_kernel(res_ref, y_ref, r_ref, gain_ref, h_ref, n_ref):
    def rows_step(i, _):
        rows = pl.ds(pl.multiple_of(i * ROWS, ROWS), ROWS)
        y = y_ref[0, rows, :].astype(f32)
        for k in range(TP - 1):
            y = y + r_ref[k, rows, :].astype(f32)
        h = res_ref[rows, :].astype(f32) + y
        mean_sq = jnp.mean(h * h, axis=-1, keepdims=True)
        h_ref[rows, :] = h.astype(bf16)
        n_ref[rows, :] = (h * lax.rsqrt(mean_sq + EPS) * gain_ref[...]).astype(bf16)
        return 0

    lax.fori_loop(0, FB // ROWS, rows_step, 0, unroll=4)


def solution(mesh):
    def local_block(x_in, w_gate, w_up, w_down, residual, norm_gain):
        D, FS = w_gate.shape
        R = residual.shape[0]
        any_ = pl.BlockSpec(memory_space=pl.ANY)
        y, r = pl.pallas_call(
            matmul_kernel,
            out_shape=(jax.ShapeDtypeStruct((TP, R, D), bf16), jax.ShapeDtypeStruct((TP - 1, R, D), bf16)),
            in_specs=[any_] * 4,
            out_specs=(any_,) * 2,
            scratch_shapes=[
                pltpu.VMEM((BIG, D), bf16),
                pltpu.VMEM((2, D, 2 * SUB), bf16),
                pltpu.VMEM((2, D, 2 * SUB), bf16),
                pltpu.VMEM((2, FS, BIG), bf16),
                pltpu.VMEM((BIG, FS), bf16),
                pltpu.VMEM((2, BIG, BIG), bf16),
                pltpu.SemaphoreType.DMA,
                pltpu.SemaphoreType.DMA((2,)),
                pltpu.SemaphoreType.DMA((2,)),
                pltpu.SemaphoreType.DMA((4,)),
                pltpu.SemaphoreType.DMA((2,)),
                pltpu.SemaphoreType.DMA((3 + TAIL,)),
                pltpu.SemaphoreType.DMA((3 + TAIL,)),
            ],
            compiler_params=pltpu.CompilerParams(collective_id=0, has_side_effects=True, vmem_limit_bytes=60 * 1024 * 1024),
            name="mlp_matmuls",
        )(x_in, w_gate, w_up, w_down)
        row_block = pl.BlockSpec((FB, D), lambda b: (b, 0))
        return pl.pallas_call(
            norm_kernel,
            grid=(R // FB,),
            out_shape=(jax.ShapeDtypeStruct((R, D), bf16), jax.ShapeDtypeStruct((R, D), bf16)),
            in_specs=[row_block, pl.BlockSpec((1, FB, D), lambda b: (TP - 1, b, 0)),
                      pl.BlockSpec((TP - 1, FB, D), lambda b: (0, b, 0)), pl.BlockSpec((1, D), lambda b: (0, 0))],
            out_specs=(row_block, row_block),
            compiler_params=pltpu.CompilerParams(vmem_limit_bytes=48 * 1024 * 1024),
            name="sum_norm",
        )(residual, y, r, norm_gain.reshape(1, D))

    row_spec = P(("data", "tp"), None)
    return jax.shard_map(local_block, mesh=mesh, in_specs=(P("data", None), P(None, "tp"), P(None, "tp"), P("tp", None), row_spec, P(None)), out_specs=(row_spec, row_spec), check_vma=False)
```

```python
import jax
import jax.numpy as jnp
from jax import lax
from jax.experimental import pallas as pl
from jax.experimental.pallas import tpu as pltpu
from jax.sharding import PartitionSpec as P

EPS = 1e-5
TP = 4
SMALL = ((0, 384, 1), (384, 640, 2))
SUB = 256
ND = 512
BIG = 1024
TAIL = 4
FB = 256
ROWS = 8

bf16 = jnp.bfloat16
f32 = jnp.float32


def matmul_kernel(x_hbm, wg_hbm, wu_hbm, wd_hbm, res_hbm, y_hbm, r_hbm, hp_hbm,
                  x_v, wg_v, wu_v, wd_v, g_v, y_v, hp_v,
                  x_sem, wg_sem, wu_sem, wd_sem, y_sem, in_sem, hp_sem, send_sem, recv_sem):
    D, FS = wg_hbm.shape
    R = y_hbm.shape[1]
    assert R == BIG
    n_gu, n_dn = FS // (2 * SUB), D // ND
    me = lax.axis_index("tp")
    far_same = lax.rem(me + 2, TP)
    far_other = TP - 1 - me
    near = me + 1 - 2 * lax.rem(me, 2)
    peers = (far_same, far_other, near)

    def owner_of(c):
        own = c // 2
        mid = (1 - own) * ((1 - c) * far_other + c * near)
        return mid + own * me

    def x_small(c):
        first, m, _ = SMALL[c]
        row = pl.multiple_of(far_same * R + first, 128)
        return pltpu.make_async_copy(x_hbm.at[pl.ds(row, m), :], x_v.at[pl.ds(0, m), :], x_sem)

    def x_big(c):
        row = pl.multiple_of(owner_of(c) * R, BIG)
        return pltpu.make_async_copy(x_hbm.at[pl.ds(row, BIG), :], x_v, x_sem)

    def gu_copies(j, slot):
        col = pl.ds(pl.multiple_of(j * 2 * SUB, 2 * SUB), 2 * SUB)
        return (pltpu.make_async_copy(wg_hbm.at[:, col], wg_v.at[slot], wg_sem.at[slot]),
                pltpu.make_async_copy(wu_hbm.at[:, col], wu_v.at[slot], wu_sem.at[slot]))

    def dn_copy(d):
        k = lax.rem(d, 4)
        at = pl.ds(pl.multiple_of(lax.rem(k, 2) * ND, ND), ND)
        return pltpu.make_async_copy(wd_hbm.at[:, pl.ds(pl.multiple_of(d * ND, ND), ND)], wd_v.at[k // 2, :, at], wd_sem.at[k])

    def dn_big(d):
        k = lax.rem(d, 2)
        return pltpu.make_async_copy(wd_hbm.at[:, pl.ds(pl.multiple_of(d * BIG, BIG), BIG)], wd_v.at[k], wd_sem.at[k])

    def y_small(c, d):
        first, m, _ = SMALL[c]
        k = lax.rem(d, 2)
        return pltpu.make_async_copy(
            y_v.at[k, pl.ds(0, m), pl.ds(0, ND)],
            y_hbm.at[0, pl.ds(first, m), pl.ds(pl.multiple_of(d * ND, ND), ND)], y_sem.at[k])

    def y_big(c, d):
        k = lax.rem(d, 2)
        return pltpu.make_async_copy(y_v.at[k], y_hbm.at[c + 1, :, pl.ds(pl.multiple_of(d * BIG, BIG), BIG)], y_sem.at[k])

    def part_copies(d):
        k = lax.rem(d + 1, 2)
        out = []
        for q in range(2):
            cols = pl.ds(pl.multiple_of(d * BIG + q * ND, ND), ND)
            top, low = pl.ds(q * BIG, BIG), pl.ds((2 + q) * BIG, BIG)
            out.append(pltpu.make_async_copy(res_hbm.at[:, cols], wg_v.at[k, top, :], in_sem.at[k, 3 * q]))
            out.append(pltpu.make_async_copy(r_hbm.at[0, :, cols], wg_v.at[k, low, :], in_sem.at[k, 3 * q + 1]))
            out.append(pltpu.make_async_copy(r_hbm.at[2, :, cols], wu_v.at[k, top, :], in_sem.at[k, 3 * q + 2]))
        return out

    def hp_copies(d):
        return [pltpu.make_async_copy(hp_v.at[q], hp_hbm.at[:, pl.ds(pl.multiple_of(d * BIG + q * ND, ND), ND)], hp_sem.at[q])
                for q in range(2)]

    def remote(slot, row, rows, cols, ssem, rsem):
        ref = (slot, pl.ds(row, rows), slice(None) if cols is None else cols)
        return pltpu.make_async_remote_copy(
            src_ref=y_hbm.at[ref], dst_ref=r_hbm.at[ref], send_sem=ssem, recv_sem=rsem,
            device_id={"tp": peers[slot]}, device_id_type=pl.DeviceIdType.MESH)

    def small_piece(c, d):
        first, m, _ = SMALL[c]
        return remote(0, first, m, pl.ds(pl.multiple_of(d * ND, ND), ND), send_sem.at[c], recv_sem.at[c])

    small_whole = [remote(0, first, m, None, send_sem.at[c], recv_sem.at[c]) for c, (first, m, _) in enumerate(SMALL)]
    rows = R // TAIL
    far_copies = [remote(1, t * rows, rows, None, send_sem.at[2 + t], recv_sem.at[2 + t]) for t in range(TAIL)]
    near_copy = remote(2, 0, R, None, send_sem.at[2 + TAIL], recv_sem.at[2 + TAIL])

    def row_parts(m, n):
        return [slice(r * (m // n), (r + 1) * (m // n)) for r in range(n)]

    def hidden(parts, slot, j):
        for q in range(2):
            cols = slice(q * SUB, (q + 1) * SUB)
            for part in parts:
                gate = jnp.dot(x_v[part, :], wg_v[slot, :, cols], preferred_element_type=f32)
                up = jnp.dot(x_v[part, :], wu_v[slot, :, cols], preferred_element_type=f32)
                g_v[part, pl.ds(pl.multiple_of(j * 2 * SUB + q * SUB, SUB), SUB)] = (gate * jax.nn.sigmoid(gate) * up).astype(bf16)

    def gate_up(parts, base, before):
        def gu_step(j, _):
            slot = lax.rem(base + j, 2)

            @pl.when(j + 1 < n_gu)
            def _():
                for cp in gu_copies(j + 1, 1 - slot):
                    cp.start()

            before(j)
            for cp in gu_copies(j, slot):
                cp.wait()
            hidden(parts, slot, j)
            return 0

        lax.fori_loop(0, n_gu, gu_step, 0)

    def small_chunk(c):
        _, m, n = SMALL[c]
        parts = row_parts(m, n)
        x_small(c).wait()

        def before(j):
            @pl.when(j >= n_gu - 3)
            def _():
                dn_copy(j - (n_gu - 3)).start()

        gate_up(parts, c * n_gu, before)

        def dn_step(d, _):
            @pl.when(d + 3 < n_dn)
            def _():
                dn_copy(d + 3).start()

            @pl.when(d == 1)
            def _():
                (x_small(1) if c == 0 else x_big(0)).start()

            @pl.when(d == 3)
            def _():
                for cp in gu_copies(0, (c + 1) * n_gu % 2):
                    cp.start()

            dn_copy(d).wait()

            @pl.when(d >= 1)
            def _():
                y_small(c, d - 1).wait()
                small_piece(c, d - 1).start()

            k = lax.rem(d, 4)
            at = pl.multiple_of(lax.rem(k, 2) * ND, ND)
            for part in parts:
                y = jnp.dot(g_v[part, :], wd_v[k // 2, :, pl.ds(at, ND)], preferred_element_type=f32)
                y_v[lax.rem(d, 2), part, 0:ND] = y.astype(bf16)
            y_small(c, d).start()
            return 0

        lax.fori_loop(0, n_dn, dn_step, 0)
        y_small(c, n_dn - 1).wait()
        small_piece(c, n_dn - 1).start()

    n_big = TP - 1
    n_wide = D // BIG

    def big_chunk(c, _):
        x_big(c).wait()

        def before(j):
            @pl.when(j == n_gu - 2)
            def _():
                dn_big(0).start()

            @pl.when((c == n_big - 1) & (j == n_gu - 1))
            def _():
                for cp in (*small_whole, near_copy):
                    cp.wait_recv()
                for cp in part_copies(0):
                    cp.start()

        gate_up(row_parts(BIG, 2), c * n_gu, before)

        def dn_step(d, _):
            @pl.when(d + 1 < n_wide)
            def _():
                dn_big(d + 1).start()

            @pl.when(d == 1)
            def _():
                x_big(c + 1).start()

            @pl.when(d == 2)
            def _():
                for cp in gu_copies(0, lax.rem((c + 1) * n_gu, 2)):
                    cp.start()

            dn_big(d).wait()

            @pl.when(d >= 1)
            def _():
                y_big(c, d - 1).wait()

            k = lax.rem(d, 2)
            for part in row_parts(BIG, 2):
                for q in range(BIG // ND):
                    cols = slice(q * ND, (q + 1) * ND)
                    y = jnp.dot(g_v[part, :], wd_v[k, :, cols], preferred_element_type=f32)
                    y_v[k, part, cols] = y.astype(bf16)
            y_big(c, d).start()
            return 0

        def own_step(d, _):
            @pl.when(d + 1 < n_wide)
            def _():
                dn_big(d + 1).start()
                for cp in part_copies(d + 1):
                    cp.start()

            dn_big(d).wait()
            for cp in part_copies(d):
                cp.wait()

            @pl.when(d >= 1)
            def _():
                for cp in hp_copies(d - 1):
                    cp.wait()

            k, t = lax.rem(d, 2), lax.rem(d + 1, 2)
            for part in row_parts(BIG, 2):
                for q in range(2):
                    cols = slice(q * ND, (q + 1) * ND)
                    at = slice(q * BIG + part.start, q * BIG + part.stop)
                    low = slice((2 + q) * BIG + part.start, (2 + q) * BIG + part.stop)
                    y = jnp.dot(g_v[part, :], wd_v[k, :, cols], preferred_element_type=f32).astype(bf16).astype(f32)
                    y = y + wg_v[t, low, :].astype(f32) + wu_v[t, at, :].astype(f32)
                    hp_v[q, part, :] = wg_v[t, at, :].astype(f32) + y
            for cp in hp_copies(d):
                cp.start()
            return 0

        @pl.when(c + 1 < n_big)
        def _():
            lax.fori_loop(0, n_wide, dn_step, 0)
            y_big(c, n_wide - 1).wait()

        @pl.when(c + 1 == n_big)
        def _():
            lax.fori_loop(0, n_wide, own_step, 0)
            for cp in hp_copies(n_wide - 1):
                cp.wait()

        @pl.when(c == 0)
        def _():
            for cp in far_copies:
                cp.start()

        @pl.when(c == 1)
        def _():
            near_copy.start()
        return 0

    for cp in gu_copies(0, 0):
        cp.start()
    x_small(0).start()
    barrier = pltpu.get_barrier_semaphore()
    for peer in peers:
        pl.semaphore_signal(barrier, inc=1, device_id={"tp": peer}, device_id_type=pl.DeviceIdType.MESH)
    pl.semaphore_wait(barrier, TP - 1)

    small_chunk(0)
    small_chunk(1)
    lax.fori_loop(0, n_big, big_chunk, 0)
    for cp in far_copies:
        cp.wait_recv()
    for cp in (*small_whole, *far_copies, near_copy):
        cp.wait_send()


def norm_kernel(hp_ref, r_ref, gain_ref, h_ref, n_ref):
    def rows_step(i, _):
        rows = pl.ds(pl.multiple_of(i * ROWS, ROWS), ROWS)
        h = hp_ref[rows, :] + r_ref[0, rows, :].astype(f32)
        mean_sq = jnp.mean(h * h, axis=-1, keepdims=True)
        h_ref[rows, :] = h.astype(bf16)
        n_ref[rows, :] = (h * lax.rsqrt(mean_sq + EPS) * gain_ref[...]).astype(bf16)
        return 0

    lax.fori_loop(0, FB // ROWS, rows_step, 0, unroll=4)


def solution(mesh):
    def local_block(x_in, w_gate, w_up, w_down, residual, norm_gain):
        D, FS = w_gate.shape
        R = residual.shape[0]
        any_ = pl.BlockSpec(memory_space=pl.ANY)
        _, r, hp = pl.pallas_call(
            matmul_kernel,
            out_shape=(jax.ShapeDtypeStruct((TP - 1, R, D), bf16), jax.ShapeDtypeStruct((TP - 1, R, D), bf16), jax.ShapeDtypeStruct((R, D), f32)),
            in_specs=[any_] * 5,
            out_specs=(any_,) * 3,
            scratch_shapes=[
                pltpu.VMEM((BIG, D), bf16),
                pltpu.VMEM((2, D, 2 * SUB), bf16),
                pltpu.VMEM((2, D, 2 * SUB), bf16),
                pltpu.VMEM((2, FS, BIG), bf16),
                pltpu.VMEM((BIG, FS), bf16),
                pltpu.VMEM((2, BIG, BIG), bf16),
                pltpu.VMEM((2, BIG, ND), f32),
                pltpu.SemaphoreType.DMA,
                pltpu.SemaphoreType.DMA((2,)),
                pltpu.SemaphoreType.DMA((2,)),
                pltpu.SemaphoreType.DMA((4,)),
                pltpu.SemaphoreType.DMA((2,)),
                pltpu.SemaphoreType.DMA((2, 6)),
                pltpu.SemaphoreType.DMA((2,)),
                pltpu.SemaphoreType.DMA((3 + TAIL,)),
                pltpu.SemaphoreType.DMA((3 + TAIL,)),
            ],
            compiler_params=pltpu.CompilerParams(collective_id=0, has_side_effects=True, vmem_limit_bytes=60 * 1024 * 1024),
            name="mlp_matmuls",
        )(x_in, w_gate, w_up, w_down, residual)
        row_block = pl.BlockSpec((FB, D), lambda b: (b, 0))
        return pl.pallas_call(
            norm_kernel,
            grid=(R // FB,),
            out_shape=(jax.ShapeDtypeStruct((R, D), bf16), jax.ShapeDtypeStruct((R, D), bf16)),
            in_specs=[row_block, pl.BlockSpec((1, FB, D), lambda b: (1, b, 0)), pl.BlockSpec((1, D), lambda b: (0, 0))],
            out_specs=(row_block, row_block),
            compiler_params=pltpu.CompilerParams(vmem_limit_bytes=48 * 1024 * 1024),
            name="sum_norm",
        )(hp, r, norm_gain.reshape(1, D))

    row_spec = P(("data", "tp"), None)
    return jax.shard_map(local_block, mesh=mesh, in_specs=(P("data", None), P(None, "tp"), P(None, "tp"), P("tp", None), row_spec, P(None)), out_specs=(row_spec, row_spec), check_vma=False)
```

```python
import jax
import jax.numpy as jnp
from jax import lax
from jax.experimental import pallas as pl
from jax.experimental.pallas import tpu as pltpu
from jax.sharding import PartitionSpec as P

EPS = 1e-5
TP = 4
SMALL = ((0, 384, 1), (384, 640, 2))
SUB = 256
ND = 512
BIG = 1024
TAIL = 4
FB = 256
ROWS = 8

bf16 = jnp.bfloat16
f32 = jnp.float32


def matmul_kernel(x_hbm, wg_hbm, wu_hbm, wd_hbm, res_hbm, y_hbm, r_hbm, hp_hbm,
                  x_v, wg_v, wu_v, wd_v, g_v, y_v, hp_v,
                  x_sem, wg_sem, wu_sem, wd_sem, y_sem, in_sem, hp_sem, send_sem, recv_sem):
    D, FS = wg_hbm.shape
    R = y_hbm.shape[1]
    assert R == BIG
    n_gu = FS // (2 * SUB)
    me = lax.axis_index("tp")
    far_same = lax.rem(me + 2, TP)
    far_other = TP - 1 - me
    near = me + 1 - 2 * lax.rem(me, 2)
    peers = (far_same, far_other, near)

    def owner_of(c):
        own = c // 2
        mid = (1 - own) * ((1 - c) * far_other + c * near)
        return mid + own * me

    def x_small(c):
        first, m, _ = SMALL[c]
        row = pl.multiple_of(far_same * R + first, 128)
        return pltpu.make_async_copy(x_hbm.at[pl.ds(row, m), :], x_v.at[pl.ds(0, m), :], x_sem)

    def x_big(c):
        row = pl.multiple_of(owner_of(c) * R, BIG)
        return pltpu.make_async_copy(x_hbm.at[pl.ds(row, BIG), :], x_v, x_sem)

    def gu_copies(j, slot):
        col = pl.ds(pl.multiple_of(j * 2 * SUB, 2 * SUB), 2 * SUB)
        return (pltpu.make_async_copy(wg_hbm.at[:, col], wg_v.at[slot], wg_sem.at[slot]),
                pltpu.make_async_copy(wu_hbm.at[:, col], wu_v.at[slot], wu_sem.at[slot]))

    def dn_big(d):
        k = lax.rem(d, 2)
        return pltpu.make_async_copy(wd_hbm.at[:, pl.ds(pl.multiple_of(d * BIG, BIG), BIG)], wd_v.at[k], wd_sem.at[k])

    def y_small(c, d):
        first, m, _ = SMALL[c]
        k = lax.rem(d, 2)
        return pltpu.make_async_copy(
            y_v.at[k, pl.ds(0, m), pl.ds(0, BIG)],
            y_hbm.at[0, pl.ds(first, m), pl.ds(pl.multiple_of(d * BIG, BIG), BIG)], y_sem.at[k])

    def y_big(c, d):
        k = lax.rem(d, 2)
        return pltpu.make_async_copy(y_v.at[k], y_hbm.at[c + 1, :, pl.ds(pl.multiple_of(d * BIG, BIG), BIG)], y_sem.at[k])

    def part_copies(d):
        k = lax.rem(d + 1, 2)
        out = []
        for q in range(2):
            cols = pl.ds(pl.multiple_of(d * BIG + q * ND, ND), ND)
            top, low = pl.ds(q * BIG, BIG), pl.ds((2 + q) * BIG, BIG)
            out.append(pltpu.make_async_copy(res_hbm.at[:, cols], wg_v.at[k, top, :], in_sem.at[k, 3 * q]))
            out.append(pltpu.make_async_copy(r_hbm.at[0, :, cols], wg_v.at[k, low, :], in_sem.at[k, 3 * q + 1]))
            out.append(pltpu.make_async_copy(r_hbm.at[2, :, cols], wu_v.at[k, top, :], in_sem.at[k, 3 * q + 2]))
        return out

    def hp_copies(d):
        return [pltpu.make_async_copy(hp_v.at[q], hp_hbm.at[:, pl.ds(pl.multiple_of(d * BIG + q * ND, ND), ND)], hp_sem.at[q])
                for q in range(2)]

    def remote(slot, row, rows, cols, ssem, rsem):
        ref = (slot, pl.ds(row, rows), slice(None) if cols is None else cols)
        return pltpu.make_async_remote_copy(
            src_ref=y_hbm.at[ref], dst_ref=r_hbm.at[ref], send_sem=ssem, recv_sem=rsem,
            device_id={"tp": peers[slot]}, device_id_type=pl.DeviceIdType.MESH)

    def small_piece(c, d):
        first, m, _ = SMALL[c]
        return remote(0, first, m, pl.ds(pl.multiple_of(d * BIG, BIG), BIG), send_sem.at[c], recv_sem.at[c])

    small_whole = [remote(0, first, m, None, send_sem.at[c], recv_sem.at[c]) for c, (first, m, _) in enumerate(SMALL)]
    rows = R // TAIL
    far_copies = [remote(1, t * rows, rows, None, send_sem.at[2 + t], recv_sem.at[2 + t]) for t in range(TAIL)]
    near_copy = remote(2, 0, R, None, send_sem.at[2 + TAIL], recv_sem.at[2 + TAIL])

    def row_parts(m, n):
        return [slice(r * (m // n), (r + 1) * (m // n)) for r in range(n)]

    def hidden(parts, slot, j):
        for q in range(2):
            cols = slice(q * SUB, (q + 1) * SUB)
            for part in parts:
                gate = jnp.dot(x_v[part, :], wg_v[slot, :, cols], preferred_element_type=f32)
                up = jnp.dot(x_v[part, :], wu_v[slot, :, cols], preferred_element_type=f32)
                g_v[part, pl.ds(pl.multiple_of(j * 2 * SUB + q * SUB, SUB), SUB)] = (gate * jax.nn.sigmoid(gate) * up).astype(bf16)

    def gate_up(parts, base, before):
        def gu_step(j, _):
            slot = lax.rem(base + j, 2)

            @pl.when(j + 1 < n_gu)
            def _():
                for cp in gu_copies(j + 1, 1 - slot):
                    cp.start()

            before(j)
            for cp in gu_copies(j, slot):
                cp.wait()
            hidden(parts, slot, j)
            return 0

        lax.fori_loop(0, n_gu, gu_step, 0)

    n_wide = D // BIG

    def small_chunk(c):
        _, m, n = SMALL[c]
        parts = row_parts(m, n)
        x_small(c).wait()

        def before(j):
            @pl.when(j == n_gu - 2)
            def _():
                dn_big(0).start()

        gate_up(parts, c * n_gu, before)

        def dn_step(d, _):
            @pl.when(d + 1 < n_wide)
            def _():
                dn_big(d + 1).start()

            @pl.when(d == 1)
            def _():
                (x_small(1) if c == 0 else x_big(0)).start()

            @pl.when(d == 2)
            def _():
                for cp in gu_copies(0, (c + 1) * n_gu % 2):
                    cp.start()

            dn_big(d).wait()

            @pl.when(d >= 1)
            def _():
                y_small(c, d - 1).wait()
                small_piece(c, d - 1).start()

            k = lax.rem(d, 2)
            for part in parts:
                for q in range(BIG // SUB):
                    cols = slice(q * SUB, (q + 1) * SUB)
                    y = jnp.dot(g_v[part, :], wd_v[k, :, cols], preferred_element_type=f32)
                    y_v[k, part, cols] = y.astype(bf16)
            y_small(c, d).start()
            return 0

        lax.fori_loop(0, n_wide, dn_step, 0)
        y_small(c, n_wide - 1).wait()
        small_piece(c, n_wide - 1).start()

    n_big = TP - 1

    def big_chunk(c, _):
        x_big(c).wait()

        def before(j):
            @pl.when(j == n_gu - 2)
            def _():
                dn_big(0).start()

            @pl.when((c == n_big - 1) & (j == n_gu - 1))
            def _():
                for cp in (*small_whole, near_copy):
                    cp.wait_recv()
                for cp in part_copies(0):
                    cp.start()

        gate_up(row_parts(BIG, 2), c * n_gu, before)

        def dn_step(d, _):
            @pl.when(d + 1 < n_wide)
            def _():
                dn_big(d + 1).start()

            @pl.when(d == 1)
            def _():
                x_big(c + 1).start()

            @pl.when(d == 2)
            def _():
                for cp in gu_copies(0, lax.rem((c + 1) * n_gu, 2)):
                    cp.start()

            dn_big(d).wait()

            @pl.when(d >= 1)
            def _():
                y_big(c, d - 1).wait()

            k = lax.rem(d, 2)
            for part in row_parts(BIG, 2):
                for q in range(BIG // SUB):
                    cols = slice(q * SUB, (q + 1) * SUB)
                    y = jnp.dot(g_v[part, :], wd_v[k, :, cols], preferred_element_type=f32)
                    y_v[k, part, cols] = y.astype(bf16)
            y_big(c, d).start()
            return 0

        def own_step(d, _):
            @pl.when(d + 1 < n_wide)
            def _():
                dn_big(d + 1).start()
                for cp in part_copies(d + 1):
                    cp.start()

            dn_big(d).wait()
            for cp in part_copies(d):
                cp.wait()

            @pl.when(d >= 1)
            def _():
                for cp in hp_copies(d - 1):
                    cp.wait()

            k, t = lax.rem(d, 2), lax.rem(d + 1, 2)
            for part in row_parts(BIG, 2):
                for q, u in ((0, 0), (0, 1), (1, 0), (1, 1)):
                    cols = slice(q * ND + u * SUB, q * ND + (u + 1) * SUB)
                    sub = slice(u * SUB, (u + 1) * SUB)
                    at = slice(q * BIG + part.start, q * BIG + part.stop)
                    low = slice((2 + q) * BIG + part.start, (2 + q) * BIG + part.stop)
                    y = jnp.dot(g_v[part, :], wd_v[k, :, cols], preferred_element_type=f32).astype(bf16).astype(f32)
                    y = y + wg_v[t, low, sub].astype(f32) + wu_v[t, at, sub].astype(f32)
                    hp_v[q, part, sub] = wg_v[t, at, sub].astype(f32) + y
            for cp in hp_copies(d):
                cp.start()
            return 0

        @pl.when(c + 1 < n_big)
        def _():
            lax.fori_loop(0, n_wide, dn_step, 0)
            y_big(c, n_wide - 1).wait()

        @pl.when(c + 1 == n_big)
        def _():
            lax.fori_loop(0, n_wide, own_step, 0)
            for cp in hp_copies(n_wide - 1):
                cp.wait()

        @pl.when(c == 0)
        def _():
            for cp in far_copies:
                cp.start()

        @pl.when(c == 1)
        def _():
            near_copy.start()
        return 0

    for cp in gu_copies(0, 0):
        cp.start()
    x_small(0).start()
    barrier = pltpu.get_barrier_semaphore()
    for peer in peers:
        pl.semaphore_signal(barrier, inc=1, device_id={"tp": peer}, device_id_type=pl.DeviceIdType.MESH)
    pl.semaphore_wait(barrier, TP - 1)

    small_chunk(0)
    small_chunk(1)
    lax.fori_loop(0, n_big, big_chunk, 0)
    for cp in far_copies:
        cp.wait_recv()
    for cp in (*small_whole, *far_copies, near_copy):
        cp.wait_send()


def norm_kernel(hp_ref, r_ref, gain_ref, h_ref, n_ref):
    def rows_step(i, _):
        rows = pl.ds(pl.multiple_of(i * ROWS, ROWS), ROWS)
        h = hp_ref[rows, :] + r_ref[0, rows, :].astype(f32)
        mean_sq = jnp.mean(h * h, axis=-1, keepdims=True)
        h_ref[rows, :] = h.astype(bf16)
        n_ref[rows, :] = (h * lax.rsqrt(mean_sq + EPS) * gain_ref[...]).astype(bf16)
        return 0

    lax.fori_loop(0, FB // ROWS, rows_step, 0, unroll=4)


def solution(mesh):
    def local_block(x_in, w_gate, w_up, w_down, residual, norm_gain):
        D, FS = w_gate.shape
        R = residual.shape[0]
        any_ = pl.BlockSpec(memory_space=pl.ANY)
        _, r, hp = pl.pallas_call(
            matmul_kernel,
            out_shape=(jax.ShapeDtypeStruct((TP - 1, R, D), bf16), jax.ShapeDtypeStruct((TP - 1, R, D), bf16), jax.ShapeDtypeStruct((R, D), f32)),
            in_specs=[any_] * 5,
            out_specs=(any_,) * 3,
            scratch_shapes=[
                pltpu.VMEM((BIG, D), bf16),
                pltpu.VMEM((2, D, 2 * SUB), bf16),
                pltpu.VMEM((2, D, 2 * SUB), bf16),
                pltpu.VMEM((2, FS, BIG), bf16),
                pltpu.VMEM((BIG, FS), bf16),
                pltpu.VMEM((2, BIG, BIG), bf16),
                pltpu.VMEM((2, BIG, ND), f32),
                pltpu.SemaphoreType.DMA,
                pltpu.SemaphoreType.DMA((2,)),
                pltpu.SemaphoreType.DMA((2,)),
                pltpu.SemaphoreType.DMA((2,)),
                pltpu.SemaphoreType.DMA((2,)),
                pltpu.SemaphoreType.DMA((2, 6)),
                pltpu.SemaphoreType.DMA((2,)),
                pltpu.SemaphoreType.DMA((3 + TAIL,)),
                pltpu.SemaphoreType.DMA((3 + TAIL,)),
            ],
            compiler_params=pltpu.CompilerParams(collective_id=0, has_side_effects=True, vmem_limit_bytes=60 * 1024 * 1024),
            name="mlp_matmuls",
        )(x_in, w_gate, w_up, w_down, residual)
        row_block = pl.BlockSpec((FB, D), lambda b: (b, 0))
        return pl.pallas_call(
            norm_kernel,
            grid=(R // FB,),
            out_shape=(jax.ShapeDtypeStruct((R, D), bf16), jax.ShapeDtypeStruct((R, D), bf16)),
            in_specs=[row_block, pl.BlockSpec((1, FB, D), lambda b: (1, b, 0)), pl.BlockSpec((1, D), lambda b: (0, 0))],
            out_specs=(row_block, row_block),
            compiler_params=pltpu.CompilerParams(vmem_limit_bytes=48 * 1024 * 1024),
            name="sum_norm",
        )(hp, r, norm_gain.reshape(1, D))

    row_spec = P(("data", "tp"), None)
    return jax.shard_map(local_block, mesh=mesh, in_specs=(P("data", None), P(None, "tp"), P(None, "tp"), P("tp", None), row_spec, P(None)), out_specs=(row_spec, row_spec), check_vma=False)
```
